128 devices in a mesh: data: 1, outer: 16 (over z, y), expert: 8 (over x, core).
Axes of the slice: x: 4, y: 4, z: 4, core: 2. Of those that a mesh axis runs over, the one named last changes fastest.
Arguments:
- tokens: bfloat16 [32768, 2048], P(('data', 'outer', 'expert'))
- w_router: bfloat16 [2048, 128], replicated
- routes: int32 [32768, 8], P(('data', 'outer', 'expert'))
- w_gate: bfloat16 [128, 2048, 768], P(('outer', 'expert'))
- w_up: bfloat16 [128, 2048, 768], P(('outer', 'expert'))
- w_down: bfloat16 [128, 768, 2048], P(('outer', 'expert'))
Outputs:
- output: bfloat16 [32768, 2048], P(('data', 'outer', 'expert'))
All inputs are finite; a program needn't handle non-finite values.
Results may differ from the reference program's by a relative error of at most 0.00827862.
Values are sent between devices in bfloat16 or wider.
A program may use at most 1 GiB of HBM per device.

```python
import jax
import jax.numpy as jnp
from jax import lax

D = 2048
FF = 768
EXPERTS = 128
TOPK = 8
TOKENS = 256
OUTER = 16
GROUP = 8
LIMIT = 4

DEVICES = OUTER * GROUP
ROWS = DEVICES * TOKENS
PER_OUTER = EXPERTS // OUTER
CAPACITY = (5 * TOKENS * TOPK + 4 * EXPERTS - 1) // (4 * EXPERTS)


def draw_routes(route_key):
    key_hot, key_grp, key_exp = jax.random.split(route_key, 3)
    score_span = 2 ** 20
    hot_dev = jax.random.randint(key_hot, (DEVICES,), 0, EXPERTS)
    hot_tok = jnp.repeat(hot_dev, TOKENS)
    forced = (jnp.arange(ROWS) % TOKENS) < CAPACITY
    outer_ids = jnp.arange(OUTER)
    grp_score = jax.random.randint(key_grp, (ROWS, OUTER), 0, score_span) * OUTER + outer_ids[None, :]
    grp_boost = forced[:, None] & (outer_ids[None, :] == (hot_tok // PER_OUTER)[:, None])
    grp_score = jnp.where(grp_boost, score_span * OUTER, grp_score)
    groups = jnp.argsort(-grp_score, axis=1)[:, :LIMIT]
    cand_count = LIMIT * PER_OUTER
    cand_ids = (groups[:, :, None] * PER_OUTER + jnp.arange(PER_OUTER)[None, None, :]).reshape(ROWS, cand_count)
    cand_score = jax.random.randint(key_exp, (ROWS, cand_count), 0, score_span) * cand_count + jnp.arange(cand_count)[None, :]
    cand_boost = forced[:, None] & (cand_ids == hot_tok[:, None])
    cand_score = jnp.where(cand_boost, score_span * cand_count, cand_score)
    pick_order = jnp.argsort(-cand_score, axis=1)[:, :TOPK]
    return jnp.take_along_axis(cand_ids, pick_order, axis=1).astype(jnp.int32)


def setup_inputs(seed: int = 0, part: int = 0) -> dict:
    base_key = jax.random.key(seed)
    part_key = jax.random.fold_in(base_key, part)
    key_tok, key_route = jax.random.split(part_key)
    key_router, key_gate, key_up, key_down = jax.random.split(base_key, 4)
    tokens = jax.random.normal(key_tok, (ROWS, D), jnp.float32).astype(jnp.bfloat16)
    w_router = (jax.random.normal(key_router, (D, EXPERTS), jnp.float32) * (2.0 / D ** 0.5)).astype(jnp.bfloat16)
    routes = draw_routes(key_route)
    w_gate = (jax.random.normal(key_gate, (EXPERTS, D, FF), jnp.float32) * D ** -0.5).astype(jnp.bfloat16)
    w_up = (jax.random.normal(key_up, (EXPERTS, D, FF), jnp.float32) * D ** -0.5).astype(jnp.bfloat16)
    w_down = (jax.random.normal(key_down, (EXPERTS, FF, D), jnp.float32) * FF ** -0.5).astype(jnp.bfloat16)
    return {'tokens': tokens, 'w_router': w_router, 'routes': routes, 'w_gate': w_gate, 'w_up': w_up, 'w_down': w_down}


def reference(tokens, w_router, routes, w_gate, w_up, w_down):
    logits = jnp.dot(tokens, w_router, preferred_element_type=jnp.float32)
    gate_vals = jax.nn.softmax(jnp.take_along_axis(logits, routes, axis=1), axis=-1)
    flat_ids = routes.reshape(DEVICES, TOKENS * TOPK)
    onehot = (flat_ids[:, :, None] == jnp.arange(EXPERTS)[None, None, :]).astype(jnp.int32)
    slot_pos = jnp.sum((jnp.cumsum(onehot, axis=1) - onehot) * onehot, axis=2)
    src_ids = jnp.arange(DEVICES)[:, None]
    total_slots = EXPERTS * DEVICES * CAPACITY
    dest_slot = jnp.where(slot_pos < CAPACITY, flat_ids * (DEVICES * CAPACITY) + src_ids * CAPACITY + slot_pos, total_slots).reshape(-1)
    pair_tok = jnp.arange(ROWS * TOPK, dtype=jnp.int32) // TOPK
    slot_tok = jnp.full((total_slots,), ROWS, jnp.int32).at[dest_slot].set(pair_tok, mode='drop')
    slot_gate = jnp.zeros((total_slots,), jnp.float32).at[dest_slot].set(gate_vals.reshape(-1), mode='drop')

    def expert_step(accum, operands):
        rows_tok, rows_gate, gate_mat, up_mat, down_mat = operands
        picked = jnp.take(tokens, rows_tok, axis=0, mode='fill', fill_value=0)
        gate_act = jnp.dot(picked, gate_mat, preferred_element_type=jnp.float32)
        up_lin = jnp.dot(picked, up_mat, preferred_element_type=jnp.float32)
        hidden = (jax.nn.silu(gate_act) * up_lin).astype(jnp.bfloat16)
        expert_out = jnp.dot(hidden, down_mat, preferred_element_type=jnp.float32).astype(jnp.bfloat16)
        accum = accum.at[rows_tok].add(rows_gate[:, None] * expert_out.astype(jnp.float32), mode='drop')
        return accum, None

    accum_init = jnp.zeros((ROWS, D), jnp.float32)
    operands = (slot_tok.reshape(EXPERTS, DEVICES * CAPACITY), slot_gate.reshape(EXPERTS, DEVICES * CAPACITY), w_gate, w_up, w_down)
    combined, _ = lax.scan(expert_step, accum_init, operands)
    return combined.astype(jnp.bfloat16)
```

```python
import functools

import jax
import jax.numpy as jnp
from jax import lax
from jax.experimental import pallas as pl
from jax.experimental.pallas import tpu as pltpu
from jax.sharding import PartitionSpec as P

MESH = pl.DeviceIdType.MESH


def local_routes(tokens, w_router, routes, num_dev, capacity):
    tok_count, top_k = routes.shape
    num_exp = w_router.shape[1]
    per_dev = num_exp // num_dev
    logits = jnp.dot(tokens, w_router, preferred_element_type=jnp.float32)
    gate_vals = jax.nn.softmax(jnp.take_along_axis(logits, routes, axis=1), axis=-1)
    flat_ids = routes.reshape(-1)
    onehot = (flat_ids[:, None] == jnp.arange(num_exp)[None, :]).astype(jnp.int32)
    slot_pos = jnp.sum((jnp.cumsum(onehot, axis=0) - onehot) * onehot, axis=1)
    total_slots = num_exp * capacity
    send_pos = (flat_ids % per_dev) * (num_dev * capacity) + (flat_ids // per_dev) * capacity + slot_pos
    dest_slot = jnp.where(slot_pos < capacity, send_pos, total_slots)
    pair_tok = jnp.arange(tok_count * top_k, dtype=jnp.int32) // top_k
    slot_tok = jnp.full((total_slots,), tok_count, jnp.int32).at[dest_slot].set(pair_tok, mode='drop')
    return gate_vals, dest_slot, slot_tok


def expert_ffn(expert_in, w_gate, w_up, w_down):
    gate_act = jnp.einsum('erd,edf->erf', expert_in, w_gate, preferred_element_type=jnp.float32)
    up_lin = jnp.einsum('erd,edf->erf', expert_in, w_up, preferred_element_type=jnp.float32)
    hidden = (jax.nn.silu(gate_act) * up_lin).astype(jnp.bfloat16)
    return jnp.einsum('erf,efd->erd', hidden, w_down, preferred_element_type=jnp.float32).astype(jnp.bfloat16)


def exchange_kernel(outer_size, group_size, src, dst, send_sem, recv_sem, self_sem):
    num_dev = outer_size * group_size
    me = lax.axis_index('outer') * group_size + lax.axis_index('expert')

    def peer(step):
        other = lax.rem(me + step, num_dev)
        return other, {'outer': other // group_size, 'expert': lax.rem(other, group_size)}

    barrier = pltpu.get_barrier_semaphore()

    def greet(step, carry):
        pl.semaphore_signal(barrier, inc=1, device_id=peer(step)[1], device_id_type=MESH)
        return carry

    lax.fori_loop(1, num_dev, greet, 0)
    pl.semaphore_wait(barrier, num_dev - 1)
    own = pltpu.make_async_copy(src.at[me], dst.at[me], self_sem)
    own.start()

    def send(step, carry):
        other, where = peer(step)
        pltpu.make_async_remote_copy(src_ref=src.at[other], dst_ref=dst.at[me], send_sem=send_sem.at[other], recv_sem=recv_sem.at[me], device_id=where, device_id_type=MESH).start()
        return carry

    lax.fori_loop(1, num_dev, send, 0)

    def finish(step, carry):
        other, where = peer(step)
        pltpu.make_async_remote_copy(src_ref=src.at[other], dst_ref=dst.at[other], send_sem=send_sem.at[other], recv_sem=recv_sem.at[other], device_id=where, device_id_type=MESH).wait()
        return carry

    lax.fori_loop(1, num_dev, finish, 0)
    own.wait()


def exchange(buf, outer_size, group_size, collective_id):
    num_dev = outer_size * group_size
    return pl.pallas_call(
        functools.partial(exchange_kernel, outer_size, group_size),
        out_shape=jax.ShapeDtypeStruct(buf.shape, buf.dtype),
        in_specs=[pl.BlockSpec(memory_space=pl.ANY)],
        out_specs=pl.BlockSpec(memory_space=pl.ANY),
        scratch_shapes=[pltpu.SemaphoreType.DMA((num_dev,)), pltpu.SemaphoreType.DMA((num_dev,)), pltpu.SemaphoreType.DMA],
        compiler_params=pltpu.CompilerParams(collective_id=collective_id, has_side_effects=True),
    )(buf)


def solution(mesh):
    outer_size = mesh.shape['outer']
    group_size = mesh.shape['expert']
    num_dev = outer_size * group_size
    row_spec = P(('data', 'outer', 'expert'), None)
    weight_spec = P(('outer', 'expert'), None, None)

    def per_device(tokens, w_router, routes, w_gate, w_up, w_down):
        tok_count, top_k = routes.shape
        model_dim = tokens.shape[1]
        num_exp = w_router.shape[1]
        per_dev = w_gate.shape[0]
        capacity = (5 * tok_count * top_k + 4 * num_exp - 1) // (4 * num_exp)
        gate_vals, dest_slot, slot_tok = local_routes(tokens, w_router, routes, num_dev, capacity)
        send_buf = jnp.take(tokens, slot_tok, axis=0, mode='fill', fill_value=0)
        recv_buf = exchange(send_buf.reshape(num_dev, capacity, model_dim), outer_size, group_size, 0)
        expert_out = expert_ffn(recv_buf.reshape(per_dev, num_dev * capacity, model_dim), w_gate, w_up, w_down)
        back_buf = exchange(expert_out.reshape(num_dev, capacity, model_dim), outer_size, group_size, 1)
        picked = jnp.take(back_buf.reshape(num_exp * capacity, model_dim), dest_slot, axis=0, mode='fill', fill_value=0)
        weighted = gate_vals[:, :, None] * picked.reshape(tok_count, top_k, model_dim).astype(jnp.float32)
        return jnp.sum(weighted, axis=1).astype(jnp.bfloat16)

    return jax.shard_map(per_device, mesh=mesh, in_specs=(row_spec, P(), row_spec, weight_spec, weight_spec, weight_spec), out_specs=row_spec, check_vma=False)
```

```python
import functools

import jax
import jax.numpy as jnp
from jax import lax
from jax.experimental import pallas as pl
from jax.experimental.pallas import tpu as pltpu
from jax.sharding import PartitionSpec as P

MESH = pl.DeviceIdType.MESH
BF16 = jnp.bfloat16
F32 = jnp.float32
NUM_DEV = 128
STRIDE = 37
GROUP = 8
NUM_GROUPS = NUM_DEV // GROUP
CAPACITY = 20
HEAD = 16
TAIL = CAPACITY - HEAD
PARTS = HEAD // TAIL
AHEAD = 4
BEHIND = 8


def iota(shape, dim):
    return lax.broadcasted_iota(jnp.int32, shape, dim)


def dot(a, b, dims=((1,), (0,))):
    return lax.dot_general(a, b, (dims, ((), ())), preferred_element_type=F32)


def moe_kernel(tokens, router, routes, gate_hbm, up_hbm, down_hbm, out, send, recv, back, w_gate, w_up, w_down, acc, place, gates, rows, hidden, tail_acc, weight_sem, send_sem, recv_sem, ret_sem, back_sem):
    tok_count, dim = tokens.shape
    num_exp = router.shape[1]
    top_k = routes.shape[1]
    part = dim // PARTS
    block = GROUP * HEAD
    outer = lax.axis_index('outer')
    line = lax.axis_index('expert')
    at_z, at_y = outer // 4, lax.rem(outer, 4)
    at_x, at_c = line // 2, lax.rem(line, 2)

    def peer(k, sign):
        m = lax.rem(k * STRIDE, NUM_DEV)
        to_z = lax.rem(at_z + 4 + sign * (m // 32), 4)
        to_y = lax.rem(at_y + 4 + sign * lax.rem(m // 8, 4), 4)
        to_x = lax.rem(at_x + 4 + sign * lax.rem(m // 2, 4), 4)
        to_c = lax.rem(at_c + 2 + sign * lax.rem(m, 2), 2)
        return {'outer': to_z * 4 + to_y, 'expert': to_x * 2 + to_c}

    def expert_of(k):
        m = (k * STRIDE) & (NUM_DEV - 1)
        to_z = (at_z + (m >> 5)) & 3
        to_y = (at_y + ((m >> 3) & 3)) & 3
        to_x = (at_x + ((m >> 1) & 3)) & 3
        to_c = (at_c + (m & 1)) & 1
        return to_z * 32 + to_y * 8 + to_x * 2 + to_c

    def dispatch(k, sign=1):
        return pltpu.make_async_remote_copy(src_ref=send.at[k], dst_ref=recv.at[k], send_sem=send_sem.at[k], recv_sem=recv_sem.at[k], device_id=peer(k, sign), device_id_type=MESH)

    def give_back(k, sign=-1):
        return pltpu.make_async_remote_copy(src_ref=recv.at[k], dst_ref=back.at[k], send_sem=ret_sem.at[k], recv_sem=back_sem.at[k], device_id=peer(k, sign), device_id_type=MESH)

    def each(group, what):
        def step(k, carry):
            what(k)
            return carry

        lax.fori_loop(lax.max(group * GROUP, 1), group * GROUP + GROUP, step, 0)

    barrier = pltpu.get_barrier_semaphore()

    def greet(k, carry):
        pl.semaphore_signal(barrier, inc=1, device_id=peer(k, 1), device_id_type=MESH)
        return carry

    lax.fori_loop(1, NUM_DEV, greet, 0)
    weights = [pltpu.make_async_copy(src, dst, weight_sem.at[n]) for n, (src, dst) in enumerate(((gate_hbm, w_gate), (up_hbm, w_up), (down_hbm, w_down)))]
    for copy in weights:
        copy.start()

    lanes = iota((tok_count, num_exp), 1)
    chosen = routes[:, 0:1] == lanes
    for j in range(1, top_k):
        chosen = chosen | (routes[:, j : j + 1] == lanes)
    earlier = (iota((tok_count, tok_count), 1) < iota((tok_count, tok_count), 0)).astype(F32).astype(BF16)
    count = dot(earlier, chosen.astype(F32).astype(BF16))
    place[...] = jnp.where(chosen, count, -1.0).astype(BF16)
    acc[...] = jnp.zeros_like(acc)
    pl.semaphore_wait(barrier, NUM_DEV - 1)

    def build(g):
        base = g * GROUP
        r = iota((block, num_exp), 0)
        pick = (expert_of(base + (r >> 4)) == iota((block, num_exp), 1)).astype(F32).astype(BF16)
        slots = dot(pick, place[...], ((1,), (1,)))
        r = iota((block, tok_count), 0)
        head = (slots == (r & (HEAD - 1)).astype(F32)).astype(F32).astype(BF16)
        in_tail = slots == (HEAD + (r & (TAIL - 1))).astype(F32)
        which = (r & (HEAD - 1)) >> 2
        tail_acc[...] = jnp.zeros_like(tail_acc)

        def column(q, carry):
            cols = pl.ds(pl.multiple_of(q * part, part), part)
            toks = tokens[:, cols]
            send[pl.ds(base, GROUP), :, cols] = dot(head, toks).astype(BF16).reshape(GROUP, HEAD, part)
            tail = jnp.where(in_tail & (which == q), 1.0, 0.0).astype(BF16)
            tail_acc[...] += dot(tail, toks)
            return carry

        lax.fori_loop(0, PARTS, column, 0)
        send[pl.ds(base, GROUP), :, dim:] = tail_acc[...].astype(BF16).reshape(GROUP, HEAD, part)

        @pl.when(g == 0)
        def _():
            recv[0] = send[0]

        each(g, lambda k: dispatch(k).start())

    def find_gates():
        lanes_chosen = place[...].astype(F32) >= 0.0
        logits = dot(tokens[...], router[...])
        top = jnp.max(jnp.where(lanes_chosen, logits, -3.0e38), axis=1, keepdims=True)
        weight = jnp.where(lanes_chosen, jnp.exp(jnp.where(lanes_chosen, logits - top, 0.0)), 0.0)
        rest = weight / jnp.sum(weight, axis=1, keepdims=True)
        for n in range(3):
            term = rest.astype(BF16)
            gates[n] = term
            rest = rest - term.astype(F32)

    def run_expert(g):
        base = g * GROUP
        each(g, lambda k: dispatch(k, -1).wait_recv())
        rows[0:block, :] = recv[pl.ds(base, GROUP), :, 0:dim].reshape(block, dim)
        tails = recv[pl.ds(base, GROUP), :, dim:].reshape(block, part)
        few = GROUP * TAIL
        i, l = iota((few, block), 0), iota((few, block), 1)
        for q in range(PARTS):
            take = (l == (i >> 2) * HEAD + q * TAIL + (i & (TAIL - 1))).astype(F32).astype(BF16)
            rows[block : block + few, q * part : (q + 1) * part] = dot(take, tails).astype(BF16)

        def up_column(n, carry):
            cols = pl.ds(pl.multiple_of(n * 256, 256), 256)
            gate = dot(rows[...], w_gate[:, cols])
            lin = dot(rows[...], w_up[:, cols])
            hidden[:, cols] = (jax.nn.silu(gate) * lin).astype(BF16)
            return carry

        lax.fori_loop(0, w_gate.shape[1] // 256, up_column, 0)
        tail_acc[...] = jnp.zeros_like(tail_acc)
        l, i = iota((block, few), 0), iota((block, few), 1)

        def down_column(q, carry):
            cols = pl.ds(pl.multiple_of(q * part, part), part)
            result = dot(hidden[...], w_down[:, cols]).astype(BF16)
            recv[pl.ds(base, GROUP), :, cols] = result[0:block].reshape(GROUP, HEAD, part)
            put = (l == (i >> 2) * HEAD + q * TAIL + (i & (TAIL - 1))).astype(F32).astype(BF16)
            tail_acc[...] += dot(put, result[block:])
            return carry

        lax.fori_loop(0, PARTS, down_column, 0)
        recv[pl.ds(base, GROUP), :, dim:] = tail_acc[...].astype(BF16).reshape(GROUP, HEAD, part)

        @pl.when(g == 0)
        def _():
            back[0] = recv[0]

        each(g, lambda k: give_back(k).start())

    def combine(g):
        base = g * GROUP
        each(g, lambda k: give_back(k, 1).wait_recv())
        l = iota((num_exp, block), 1)
        pick = (expert_of(base + (l >> 4)) == iota((num_exp, block), 0)).astype(F32).astype(BF16)
        slots = dot(place[...], pick)
        l = iota((tok_count, block), 1)
        in_head = slots == (l & (HEAD - 1)).astype(F32)
        in_tail = slots == (HEAD + (l & (TAIL - 1))).astype(F32)
        which = (l & (HEAD - 1)) >> 2
        spread = [dot(gates[n], pick) for n in range(3)]
        heads = jnp.concatenate([jnp.where(in_head, s, 0.0).astype(BF16) for s in spread], axis=0)
        tails = jnp.concatenate([jnp.where(in_tail, s, 0.0).astype(BF16) for s in spread], axis=0)
        which = jnp.concatenate([which] * 3, axis=0)

        def column(q, carry):
            cols = pl.ds(pl.multiple_of(q * part, part), part)
            total = dot(heads, back[pl.ds(base, GROUP), :, cols].reshape(block, part))
            mine = jnp.where(which == q, tails.astype(F32), 0.0).astype(BF16)
            total += dot(mine, back[pl.ds(base, GROUP), :, dim:].reshape(block, part))
            acc[:, cols] += total[0:tok_count] + (total[tok_count : 2 * tok_count] + total[2 * tok_count :])
            return carry

        lax.fori_loop(0, PARTS, column, 0)

    def step(i, carry):
        @pl.when(i < NUM_GROUPS)
        def _():
            @pl.when(i >= AHEAD)
            def _():
                each(i - AHEAD, lambda k: dispatch(k).wait_send())

            build(i)

        @pl.when(i == 2)
        def _():
            find_gates()

        @pl.when(i == AHEAD)
        def _():
            for copy in weights:
                copy.wait()

        @pl.when((i >= AHEAD) & (i < NUM_GROUPS + AHEAD))
        def _():
            run_expert(i - AHEAD)

        @pl.when(i >= BEHIND)
        def _():
            combine(i - BEHIND)

        return carry

    lax.fori_loop(0, NUM_GROUPS + BEHIND, step, 0)
    out[...] = acc[...].astype(BF16)

    def drain(k, carry):
        give_back(k).wait_send()
        return carry

    lax.fori_loop(1, NUM_DEV, drain, 0)

    def drain_send(k, carry):
        dispatch(k).wait_send()
        return carry

    lax.fori_loop((NUM_GROUPS - AHEAD) * GROUP, NUM_DEV, drain_send, 0)


def solution(mesh):
    row_spec = P(('data', 'outer', 'expert'), None)
    weight_spec = P(('outer', 'expert'), None, None)

    def per_device(tokens, w_router, routes, w_gate, w_up, w_down):
        tok_count, dim = tokens.shape
        num_exp = w_router.shape[1]
        ff = w_gate.shape[2]
        width = dim + dim // PARTS
        few = GROUP * CAPACITY
        vmem = pl.BlockSpec(memory_space=pltpu.VMEM)
        hbm = pl.BlockSpec(memory_space=pl.ANY)
        dma = pltpu.SemaphoreType.DMA
        return pl.pallas_call(
            moe_kernel,
            out_shape=jax.ShapeDtypeStruct((tok_count, dim), BF16),
            in_specs=[vmem, vmem, vmem, hbm, hbm, hbm],
            out_specs=vmem,
            scratch_shapes=[
                pltpu.VMEM((NUM_DEV, HEAD, width), BF16),
                pltpu.VMEM((NUM_DEV, HEAD, width), BF16),
                pltpu.VMEM((NUM_DEV, HEAD, width), BF16),
                pltpu.VMEM((dim, ff), BF16),
                pltpu.VMEM((dim, ff), BF16),
                pltpu.VMEM((ff, dim), BF16),
                pltpu.VMEM((tok_count, dim), F32),
                pltpu.VMEM((tok_count, num_exp), BF16),
                pltpu.VMEM((3, tok_count, num_exp), BF16),
                pltpu.VMEM((few, dim), BF16),
                pltpu.VMEM((few, ff), BF16),
                pltpu.VMEM((GROUP * HEAD, dim // PARTS), F32),
                dma((3,)),
                dma((NUM_DEV,)),
                dma((NUM_DEV,)),
                dma((NUM_DEV,)),
                dma((NUM_DEV,)),
            ],
            compiler_params=pltpu.CompilerParams(collective_id=0, has_side_effects=True, vmem_limit_bytes=63 * 2**20),
        )(tokens, w_router, routes, w_gate[0], w_up[0], w_down[0])

    return jax.shard_map(per_device, mesh=mesh, in_specs=(row_spec, P(), row_spec, weight_spec, weight_spec, weight_spec), out_specs=row_spec, check_vma=False)
```

```python
import functools

import jax
import jax.numpy as jnp
from jax import lax
from jax.experimental import pallas as pl
from jax.experimental.pallas import tpu as pltpu
from jax.sharding import PartitionSpec as P

MESH = pl.DeviceIdType.MESH
BF16 = jnp.bfloat16
F32 = jnp.float32
NUM_DEV = 128
STRIDE = 37
MIX = 1
FLIP = 1
GROUP = 8
NUM_GROUPS = NUM_DEV // GROUP
CAPACITY = 20
HEAD = 16
TAIL = CAPACITY - HEAD
PARTS = HEAD // TAIL
AHEAD = 4
BEHIND = 8


def iota(shape, dim):
    return lax.broadcasted_iota(jnp.int32, shape, dim)


def dot(a, b, dims=((1,), (0,))):
    return lax.dot_general(a, b, (dims, ((), ())), preferred_element_type=F32)


def moe_kernel(tokens, router, routes, gate_hbm, up_hbm, down_hbm, out, send, recv, back, w_gate, w_up, w_down, acc, place_t, place, gates, rows, hidden, tail_acc, ready, weight_sem, send_sem, recv_sem, ret_sem, back_sem):
    tok_count, dim = tokens.shape
    num_exp = router.shape[1]
    top_k = routes.shape[0]
    part = dim // PARTS
    block = GROUP * HEAD
    outer = lax.axis_index('outer')
    line = lax.axis_index('expert')
    at_z, at_y = outer // 4, lax.rem(outer, 4)
    at_x, at_c = line // 2, lax.rem(line, 2)

    def peer(k, sign):
        m = lax.rem(k * STRIDE, NUM_DEV)
        to_c = lax.rem(at_c + m, 2)
        turn = sign * (1 - 2 * FLIP * (at_c if sign > 0 else to_c))
        shift_x = lax.rem(m // 2, 4)
        shift_y = lax.rem(m // 8 + MIX * shift_x, 4)
        shift_z = lax.rem(m // 32 + MIX * shift_x, 4)
        to_z = lax.rem(at_z + 4 + turn * shift_z, 4)
        to_y = lax.rem(at_y + 4 + turn * shift_y, 4)
        to_x = lax.rem(at_x + 4 + turn * shift_x, 4)
        return {'outer': to_z * 4 + to_y, 'expert': to_x * 2 + to_c}

    def expert_of(k):
        m = (k * STRIDE) & (NUM_DEV - 1)
        turn = 1 - 2 * FLIP * at_c
        shift_x = (m >> 1) & 3
        to_z = (at_z + turn * ((m >> 5) + MIX * shift_x)) & 3
        to_y = (at_y + turn * ((m >> 3) + MIX * shift_x)) & 3
        to_x = (at_x + turn * shift_x) & 3
        to_c = (at_c + m) & 1
        return to_z * 32 + to_y * 8 + to_x * 2 + to_c

    def dispatch(k, sign=1):
        return pltpu.make_async_remote_copy(src_ref=send.at[k], dst_ref=recv.at[k], send_sem=send_sem.at[k], recv_sem=recv_sem.at[k], device_id=peer(k, sign), device_id_type=MESH)

    def give_back(k, sign=-1):
        return pltpu.make_async_remote_copy(src_ref=recv.at[k], dst_ref=back.at[k], send_sem=ret_sem.at[k], recv_sem=back_sem.at[k], device_id=peer(k, sign), device_id_type=MESH)

    def each(group, what):
        def step(k, carry):
            what(k)
            return carry

        lax.fori_loop(lax.max(group * GROUP, 1), group * GROUP + GROUP, step, 0)

    lines = lax.axis_size('expert')
    outers = lax.axis_size('outer')
    barrier = pltpu.get_barrier_semaphore()

    def in_line(n):
        return {'outer': outer, 'expert': lax.rem(line + n, lines)}

    for n in range(1, lines):
        pl.semaphore_signal(barrier, inc=1, device_id=in_line(n), device_id_type=MESH)
    for n in range(1, outers):
        pl.semaphore_signal(barrier, inc=1, device_id={'outer': lax.rem(outer + n, outers), 'expert': line}, device_id_type=MESH)
    weights = [pltpu.make_async_copy(src, dst, weight_sem.at[n]) for n, (src, dst) in enumerate(((gate_hbm, w_gate), (up_hbm, w_up), (down_hbm, w_down)))]
    for copy in weights:
        copy.start()

    kinds = iota((num_exp, tok_count), 0)
    chosen = routes[0:1, :] == kinds
    for j in range(1, top_k):
        chosen = chosen | (routes[j : j + 1, :] == kinds)
    square = (tok_count, tok_count)
    earlier = (iota(square, 0) < iota(square, 1)).astype(F32).astype(BF16)
    count = dot(chosen.astype(F32).astype(BF16), earlier)
    place_t[...] = jnp.where(chosen, count, -1.0).astype(BF16)
    pl.semaphore_wait(barrier, lines + outers - 2)
    for n in range(1, lines):
        pl.semaphore_signal(ready, inc=1, device_id=in_line(n), device_id_type=MESH)

    def build(g):
        base = g * GROUP
        r = iota((block, num_exp), 0)
        pick = (expert_of(base + (r >> 4)) == iota((block, num_exp), 1)).astype(F32).astype(BF16)
        slots = dot(pick, place_t[...])
        r = iota((block, tok_count), 0)
        head = (slots == (r & (HEAD - 1)).astype(F32)).astype(F32).astype(BF16)
        in_tail = slots == (HEAD + (r & (TAIL - 1))).astype(F32)
        which = (r & (HEAD - 1)) >> 2
        tail_acc[...] = jnp.zeros_like(tail_acc)

        def column(q, carry):
            cols = pl.ds(pl.multiple_of(q * part, part), part)
            toks = tokens[:, cols]
            send[pl.ds(base, GROUP), :, cols] = dot(head, toks).astype(BF16).reshape(GROUP, HEAD, part)
            tail = jnp.where(in_tail & (which == q), 1.0, 0.0).astype(BF16)
            tail_acc[...] += dot(tail, toks)
            return carry

        lax.fori_loop(0, PARTS, column, 0)
        send[pl.ds(base, GROUP), :, dim:] = tail_acc[...].astype(BF16).reshape(GROUP, HEAD, part)

    def start_group(g):
        each(g, lambda k: dispatch(k).start())

    def find_gates():
        same = (iota(square, 0) == iota(square, 1)).astype(F32).astype(BF16)
        place[...] = dot(same, place_t[...], ((1,), (1,))).astype(BF16)
        acc[...] = jnp.zeros_like(acc)
        lanes_chosen = place[...].astype(F32) >= 0.0
        logits = dot(tokens[...], router[...])
        top = jnp.max(jnp.where(lanes_chosen, logits, -3.0e38), axis=1, keepdims=True)
        weight = jnp.where(lanes_chosen, jnp.exp(jnp.where(lanes_chosen, logits - top, 0.0)), 0.0)
        rest = weight / jnp.sum(weight, axis=1, keepdims=True)
        for n in range(3):
            term = rest.astype(BF16)
            gates[n] = term
            rest = rest - term.astype(F32)

    def run_expert(g):
        base = g * GROUP
        each(g, lambda k: dispatch(k, -1).wait_recv())
        rows[0:block, :] = recv[pl.ds(base, GROUP), :, 0:dim].reshape(block, dim)
        tails = recv[pl.ds(base, GROUP), :, dim:].reshape(block, part)
        few = GROUP * TAIL
        i, l = iota((few, block), 0), iota((few, block), 1)
        for q in range(PARTS):
            take = (l == (i >> 2) * HEAD + q * TAIL + (i & (TAIL - 1))).astype(F32).astype(BF16)
            rows[block : block + few, q * part : (q + 1) * part] = dot(take, tails).astype(BF16)

        def up_column(n, carry):
            cols = pl.ds(pl.multiple_of(n * 256, 256), 256)
            gate = dot(rows[...], w_gate[:, cols])
            lin = dot(rows[...], w_up[:, cols])
            hidden[:, cols] = (jax.nn.silu(gate) * lin).astype(BF16)
            return carry

        lax.fori_loop(0, w_gate.shape[1] // 256, up_column, 0)
        tail_acc[...] = jnp.zeros_like(tail_acc)
        l, i = iota((block, few), 0), iota((block, few), 1)

        def down_column(q, carry):
            cols = pl.ds(pl.multiple_of(q * part, part), part)
            result = dot(hidden[...], w_down[:, cols]).astype(BF16)
            recv[pl.ds(base, GROUP), :, cols] = result[0:block].reshape(GROUP, HEAD, part)
            put = (l == (i >> 2) * HEAD + q * TAIL + (i & (TAIL - 1))).astype(F32).astype(BF16)
            tail_acc[...] += dot(put, result[block:])
            return carry

        lax.fori_loop(0, PARTS, down_column, 0)
        recv[pl.ds(base, GROUP), :, dim:] = tail_acc[...].astype(BF16).reshape(GROUP, HEAD, part)

        @pl.when(g == 0)
        def _():
            back[0] = recv[0]

        each(g, lambda k: give_back(k).start())

    def combine(g):
        base = g * GROUP
        l = iota((num_exp, block), 1)
        pick = (expert_of(base + (l >> 4)) == iota((num_exp, block), 0)).astype(F32).astype(BF16)
        slots = dot(place[...], pick)
        l = iota((tok_count, block), 1)
        in_head = slots == (l & (HEAD - 1)).astype(F32)
        in_tail = slots == (HEAD + (l & (TAIL - 1))).astype(F32)
        which = (l & (HEAD - 1)) >> 2
        spread = [dot(gates[n], pick) for n in range(3)]
        heads = jnp.concatenate([jnp.where(in_head, s, 0.0).astype(BF16) for s in spread], axis=0)
        tails = jnp.concatenate([jnp.where(in_tail, s, 0.0).astype(BF16) for s in spread], axis=0)
        which = jnp.concatenate([which] * 3, axis=0)
        each(g, lambda k: give_back(k, 1).wait_recv())

        def column(q, carry):
            cols = pl.ds(pl.multiple_of(q * part, part), part)
            total = dot(heads, back[pl.ds(base, GROUP), :, cols].reshape(block, part))
            mine = jnp.where(which == q, tails.astype(F32), 0.0).astype(BF16)
            total += dot(mine, back[pl.ds(base, GROUP), :, dim:].reshape(block, part))
            acc[:, cols] += total[0:tok_count] + (total[tok_count : 2 * tok_count] + total[2 * tok_count :])
            return carry

        lax.fori_loop(0, PARTS, column, 0)

    build(0)
    recv[0] = send[0]
    pl.semaphore_wait(ready, lines - 1)
    start_group(0)

    def step(i, carry):
        @pl.when((i > 0) & (i < NUM_GROUPS))
        def _():
            @pl.when(i >= AHEAD)
            def _():
                each(i - AHEAD, lambda k: dispatch(k).wait_send())

            build(i)
            start_group(i)

        @pl.when(i == 2)
        def _():
            find_gates()

        @pl.when(i == AHEAD)
        def _():
            for copy in weights:
                copy.wait()

        @pl.when((i >= AHEAD) & (i < NUM_GROUPS + AHEAD))
        def _():
            run_expert(i - AHEAD)

        @pl.when(i >= BEHIND)
        def _():
            combine(i - BEHIND)

        return carry

    lax.fori_loop(0, NUM_GROUPS + BEHIND, step, 0)
    out[...] = acc[...].astype(BF16)

    def drain(k, carry):
        give_back(k).wait_send()
        return carry

    lax.fori_loop(1, NUM_DEV, drain, 0)

    def drain_send(k, carry):
        dispatch(k).wait_send()
        return carry

    lax.fori_loop((NUM_GROUPS - AHEAD) * GROUP, NUM_DEV, drain_send, 0)


def solution(mesh):
    row_spec = P(('data', 'outer', 'expert'), None)
    weight_spec = P(('outer', 'expert'), None, None)

    def per_device(tokens, w_router, routes, w_gate, w_up, w_down):
        tok_count, dim = tokens.shape
        num_exp = w_router.shape[1]
        ff = w_gate.shape[2]
        width = dim + dim // PARTS
        few = GROUP * CAPACITY
        vmem = pl.BlockSpec(memory_space=pltpu.VMEM)
        hbm = pl.BlockSpec(memory_space=pl.ANY)
        dma = pltpu.SemaphoreType.DMA
        return pl.pallas_call(
            moe_kernel,
            out_shape=jax.ShapeDtypeStruct((tok_count, dim), BF16),
            in_specs=[vmem, vmem, vmem, hbm, hbm, hbm],
            out_specs=vmem,
            scratch_shapes=[
                pltpu.VMEM((NUM_DEV, HEAD, width), BF16),
                pltpu.VMEM((NUM_DEV, HEAD, width), BF16),
                pltpu.VMEM((NUM_DEV, HEAD, width), BF16),
                pltpu.VMEM((dim, ff), BF16),
                pltpu.VMEM((dim, ff), BF16),
                pltpu.VMEM((ff, dim), BF16),
                pltpu.VMEM((tok_count, dim), F32),
                pltpu.VMEM((num_exp, tok_count), BF16),
                pltpu.VMEM((tok_count, num_exp), BF16),
                pltpu.VMEM((3, tok_count, num_exp), BF16),
                pltpu.VMEM((few, dim), BF16),
                pltpu.VMEM((few, ff), BF16),
                pltpu.VMEM((GROUP * HEAD, dim // PARTS), F32),
                pltpu.SemaphoreType.REGULAR,
                dma((3,)),
                dma((NUM_DEV,)),
                dma((NUM_DEV,)),
                dma((NUM_DEV,)),
                dma((NUM_DEV,)),
            ],
            compiler_params=pltpu.CompilerParams(collective_id=0, has_side_effects=True, vmem_limit_bytes=63 * 2**20),
        )(tokens, w_router, routes.T, w_gate[0], w_up[0], w_down[0])

    return jax.shard_map(per_device, mesh=mesh, in_specs=(row_spec, P(), row_spec, weight_spec, weight_spec, weight_spec), out_specs=row_spec, check_vma=False)
```

```python
import functools

import jax
import jax.numpy as jnp
from jax import lax
from jax.experimental import pallas as pl
from jax.experimental.pallas import tpu as pltpu
from jax.sharding import PartitionSpec as P

MESH = pl.DeviceIdType.MESH
BF16 = jnp.bfloat16
F32 = jnp.float32
NUM_DEV = 128
SHIFTS = (0, 1, 4, 3, 12, 5, 15, 2, 8, 7, 13, 6, 9, 14, 11, 10)
GROUP = 8
NUM_GROUPS = NUM_DEV // GROUP
CAPACITY = 20
HEAD = 16
TAIL = CAPACITY - HEAD
PARTS = HEAD // TAIL
FORWARD = 2
EXPERT = 4
RETURN = 7
COMBINE = 10

def iota(shape, dim):
    return lax.broadcasted_iota(jnp.int32, shape, dim)


def dot(a, b, dims=((1,), (0,))):
    return lax.dot_general(a, b, (dims, ((), ())), preferred_element_type=F32)


def moe_kernel(tokens, router, routes, gate_hbm, up_hbm, down_hbm, out, mid, send, recv, back_mid, back, w_gate, w_up, w_down, acc, place_t, place, gates, rows, hidden, tail_acc, weight_sem, send_sem, recv_sem, ret_sem, ret_mid_sem, line_sem, mid_sem, line_ret_sem, back_sem):
    tok_count, dim = tokens.shape
    num_exp = router.shape[1]
    top_k = routes.shape[0]
    part = dim // PARTS
    block = GROUP * HEAD
    outer = lax.axis_index('outer')
    line = lax.axis_index('expert')
    at_z, at_y = outer // 4, lax.rem(outer, 4)
    at_x, at_c = line // 2, lax.rem(line, 2)

    def line_shift(g):
        other = g // (2 * 4)
        n = lax.rem(g // 2 + other, 4)
        return n + n // 2 - 2 * (n // 3), other

    def line_peer(g, sign):
        shift_x, shift_c = line_shift(g)
        return {'outer': outer, 'expert': lax.rem(at_x + 4 + sign * shift_x, 4) * 2 + lax.rem(at_c + shift_c, 2)}

    def outer_at(g, i, sign, core):
        shift = SHIFTS[i] + lax.rem(g, 2) * (SHIFTS[GROUP + i] - SHIFTS[i])
        turn = sign * (1 - 2 * core)
        to_z = lax.rem(at_z + 4 + turn * (shift // 4), 4)
        to_y = lax.rem(at_y + 4 + turn * lax.rem(shift, 4), 4)
        return to_z * 4 + to_y

    def plane_peer(g, i, sign):
        return {'outer': outer_at(g, i, sign, at_c), 'expert': line}

    def experts_of(g, which):
        shift_x, shift_c = line_shift(g)
        to_c = lax.rem(at_c + shift_c, 2)
        to_line = lax.rem(at_x + shift_x, 4) * 2 + to_c
        found = jnp.zeros_like(which)
        for i in range(GROUP):
            found = jnp.where(which == i, outer_at(g, i, 1, to_c) * 8 + to_line, found)
        return found

    def copy(src, dst, sent, got, where):
        return pltpu.make_async_remote_copy(src_ref=src, dst_ref=dst, send_sem=sent, recv_sem=got, device_id=where, device_id_type=MESH)

    def span(g, first):
        return pl.ds(g * GROUP + first, GROUP - first)

    def line_out(g, first):
        return copy(send.at[span(g, first)], mid.at[span(g, first)], line_sem.at[g], mid_sem.at[g], line_peer(g, 1))

    def line_back(g, first):
        return copy(back_mid.at[span(g, first)], back.at[span(g, first)], line_ret_sem.at[g], back_sem.at[g], line_peer(g, -1))

    def final_out(k, src, where):
        return copy(src.at[k], recv.at[k], send_sem.at[k], recv_sem.at[k], where)

    def first_back(k, dst, where):
        return copy(recv.at[k], dst.at[k], ret_sem.at[k], ret_mid_sem.at[k], where)

    def by_half(g, what):
        @pl.when(lax.rem(g, 2) == 0)
        def _():
            what(1)

        @pl.when(lax.rem(g, 2) == 1)
        def _():
            what(0)

    def each(g, what):
        def step(k, carry):
            what(k)
            return carry

        lax.fori_loop(lax.max(g * GROUP, 1), g * GROUP + GROUP, step, 0)

    lines = lax.axis_size('expert')
    outers = lax.axis_size('outer')
    barrier = pltpu.get_barrier_semaphore()

    for n in range(1, lines):
        pl.semaphore_signal(barrier, inc=1, device_id={'outer': outer, 'expert': lax.rem(line + n, lines)}, device_id_type=MESH)
    for n in range(1, outers):
        pl.semaphore_signal(barrier, inc=1, device_id={'outer': lax.rem(outer + n, outers), 'expert': line}, device_id_type=MESH)
    weights = [pltpu.make_async_copy(src, dst, weight_sem.at[n]) for n, (src, dst) in enumerate(((gate_hbm, w_gate), (up_hbm, w_up), (down_hbm, w_down)))]
    for load in weights:
        load.start()

    kinds = iota((num_exp, tok_count), 0)
    chosen = routes[0:1, :] == kinds
    for j in range(1, top_k):
        chosen = chosen | (routes[j : j + 1, :] == kinds)
    square = (tok_count, tok_count)
    earlier = (iota(square, 0) < iota(square, 1)).astype(F32).astype(BF16)
    count = dot(chosen.astype(F32).astype(BF16), earlier)
    place_t[...] = jnp.where(chosen, count, -1.0).astype(BF16)

    def build(g):
        base = g * GROUP
        r = iota((block, num_exp), 0)
        pick = (experts_of(g, r >> 4) == iota((block, num_exp), 1)).astype(F32).astype(BF16)
        slots = dot(pick, place_t[...])
        r = iota((block, tok_count), 0)
        head = (slots == (r & (HEAD - 1)).astype(F32)).astype(F32).astype(BF16)
        in_tail = slots == (HEAD + (r & (TAIL - 1))).astype(F32)
        which = (r & (HEAD - 1)) >> 2
        tail_acc[...] = jnp.zeros_like(tail_acc)

        def column(q, carry):
            cols = pl.ds(pl.multiple_of(q * part, part), part)
            toks = tokens[:, cols]
            send[pl.ds(base, GROUP), :, cols] = dot(head, toks).astype(BF16).reshape(GROUP, HEAD, part)
            tail = jnp.where(in_tail & (which == q), 1.0, 0.0).astype(BF16)
            tail_acc[...] += dot(tail, toks)
            return carry

        lax.fori_loop(0, PARTS, column, 0)
        send[pl.ds(base, GROUP), :, dim:] = tail_acc[...].astype(BF16).reshape(GROUP, HEAD, part)

    def start_group(g):
        base = g * GROUP

        def direct(first):
            for i in range(first, GROUP):
                final_out(base + i, send, plane_peer(g, i, 1)).start()

        def hop(first):
            line_out(g, first).start()
            if first:
                final_out(base, send, line_peer(g, 1)).start()

        @pl.when(g < 2)
        def _():
            by_half(g, direct)

        @pl.when(g >= 2)
        def _():
            by_half(g, hop)

    def forward(g):
        def pass_on(first):
            line_out(g, first).wait_recv()
            for i in range(first, GROUP):
                final_out(g * GROUP + i, mid, plane_peer(g, i, 1)).start()

        by_half(g, pass_on)

    def find_gates():
        same = (iota(square, 0) == iota(square, 1)).astype(F32).astype(BF16)
        place[...] = dot(same, place_t[...], ((1,), (1,))).astype(BF16)
        acc[...] = jnp.zeros_like(acc)
        lanes_chosen = place[...].astype(F32) >= 0.0
        logits = dot(tokens[...], router[...])
        top = jnp.max(jnp.where(lanes_chosen, logits, -3.0e38), axis=1, keepdims=True)
        weight = jnp.where(lanes_chosen, jnp.exp(jnp.where(lanes_chosen, logits - top, 0.0)), 0.0)
        rest = weight / jnp.sum(weight, axis=1, keepdims=True)
        for n in range(3):
            term = rest.astype(BF16)
            gates[n] = term
            rest = rest - term.astype(F32)

    def run_expert(g):
        base = g * GROUP
        each(g, lambda k: final_out(k, send, line_peer(2, 1)).wait_recv())
        rows[0:block, :] = recv[pl.ds(base, GROUP), :, 0:dim].reshape(block, dim)
        tails = recv[pl.ds(base, GROUP), :, dim:].reshape(block, part)
        few = GROUP * TAIL
        i, l = iota((few, block), 0), iota((few, block), 1)
        for q in range(PARTS):
            take = (l == (i >> 2) * HEAD + q * TAIL + (i & (TAIL - 1))).astype(F32).astype(BF16)
            rows[block : block + few, q * part : (q + 1) * part] = dot(take, tails).astype(BF16)

        def up_column(n, carry):
            cols = pl.ds(pl.multiple_of(n * 256, 256), 256)
            gate = dot(rows[...], w_gate[:, cols])
            lin = dot(rows[...], w_up[:, cols])
            hidden[:, cols] = (jax.nn.silu(gate) * lin).astype(BF16)
            return carry

        lax.fori_loop(0, w_gate.shape[1] // 256, up_column, 0)
        tail_acc[...] = jnp.zeros_like(tail_acc)
        l, i = iota((block, few), 0), iota((block, few), 1)

        def down_column(q, carry):
            cols = pl.ds(pl.multiple_of(q * part, part), part)
            result = dot(hidden[...], w_down[:, cols]).astype(BF16)
            recv[pl.ds(base, GROUP), :, cols] = result[0:block].reshape(GROUP, HEAD, part)
            put = (l == (i >> 2) * HEAD + q * TAIL + (i & (TAIL - 1))).astype(F32).astype(BF16)
            tail_acc[...] += dot(put, result[block:])
            return carry

        lax.fori_loop(0, PARTS, down_column, 0)
        recv[pl.ds(base, GROUP), :, dim:] = tail_acc[...].astype(BF16).reshape(GROUP, HEAD, part)

        @pl.when(g == 0)
        def _():
            back[0] = recv[0]

        def give(first, dst):
            for i in range(first, GROUP):
                first_back(base + i, dst, plane_peer(g, i, -1)).start()

        def hop(first):
            if first:
                first_back(base, back, line_peer(g, -1)).start()
            give(first, back_mid)

        @pl.when(g < 2)
        def _():
            by_half(g, lambda first: give(first, back))

        @pl.when(g >= 2)
        def _():
            by_half(g, hop)

    def hand_on(g):
        def pass_on(first):
            for i in range(first, GROUP):
                first_back(g * GROUP + i, back_mid, line_peer(g, -1)).wait_recv()
            line_back(g, first).start()

        by_half(g, pass_on)

    def combine(g):
        base = g * GROUP
        l = iota((num_exp, block), 1)
        pick = (experts_of(g, l >> 4) == iota((num_exp, block), 0)).astype(F32).astype(BF16)
        slots = dot(place[...], pick)
        l = iota((tok_count, block), 1)
        in_head = slots == (l & (HEAD - 1)).astype(F32)
        in_tail = slots == (HEAD + (l & (TAIL - 1))).astype(F32)
        which = (l & (HEAD - 1)) >> 2
        spread = [dot(gates[n], pick) for n in range(3)]
        heads = jnp.concatenate([jnp.where(in_head, s, 0.0).astype(BF16) for s in spread], axis=0)
        tails = jnp.concatenate([jnp.where(in_tail, s, 0.0).astype(BF16) for s in spread], axis=0)
        which = jnp.concatenate([which] * 3, axis=0)

        @pl.when(g < 2)
        def _():
            each(g, lambda k: first_back(k, back, line_peer(2, -1)).wait_recv())

        def arrive(first):
            line_back(g, first).wait_recv()
            if first:
                first_back(base, back, line_peer(g, -1)).wait_recv()

        @pl.when(g >= 2)
        def _():
            by_half(g, arrive)


        def column(q, carry):
            cols = pl.ds(pl.multiple_of(q * part, part), part)
            total = dot(heads, back[pl.ds(base, GROUP), :, cols].reshape(block, part))
            mine = jnp.where(which == q, tails.astype(F32), 0.0).astype(BF16)
            total += dot(mine, back[pl.ds(base, GROUP), :, dim:].reshape(block, part))
            acc[:, cols] += total[0:tok_count] + (total[tok_count : 2 * tok_count] + total[2 * tok_count :])
            return carry

        lax.fori_loop(0, PARTS, column, 0)

    build(0)
    recv[0] = send[0]
    pl.semaphore_wait(barrier, lines + outers - 2)
    start_group(0)

    def step(i, carry):
        @pl.when((i > 0) & (i < NUM_GROUPS))
        def _():
            build(i)
            start_group(i)

        @pl.when((i >= FORWARD + 2) & (i < NUM_GROUPS + FORWARD))
        def _():
            forward(i - FORWARD)

        @pl.when(i == 2)
        def _():
            find_gates()

        @pl.when(i == EXPERT)
        def _():
            for load in weights:
                load.wait()

        @pl.when((i >= EXPERT) & (i < NUM_GROUPS + EXPERT))
        def _():
            run_expert(i - EXPERT)

        @pl.when((i >= RETURN + 2) & (i < NUM_GROUPS + RETURN))
        def _():
            hand_on(i - RETURN)

        @pl.when(i >= COMBINE)
        def _():
            combine(i - COMBINE)

        return carry

    lax.fori_loop(0, NUM_GROUPS + COMBINE, step, 0)
    out[...] = acc[...].astype(BF16)

    def drain(k, carry):
        final_out(k, send, line_peer(2, 1)).wait_send()
        first_back(k, back, line_peer(2, -1)).wait_send()
        return carry

    lax.fori_loop(1, NUM_DEV, drain, 0)

    def drain_line(g, carry):
        def drained(first):
            line_out(g, first).wait_send()
            line_back(g, first).wait_send()

        by_half(g, drained)
        return carry

    lax.fori_loop(2, NUM_GROUPS, drain_line, 0)


def solution(mesh):
    row_spec = P(('data', 'outer', 'expert'), None)
    weight_spec = P(('outer', 'expert'), None, None)

    def per_device(tokens, w_router, routes, w_gate, w_up, w_down):
        tok_count, dim = tokens.shape
        num_exp = w_router.shape[1]
        ff = w_gate.shape[2]
        width = dim + dim // PARTS
        few = GROUP * CAPACITY
        vmem = pl.BlockSpec(memory_space=pltpu.VMEM)
        hbm = pl.BlockSpec(memory_space=pl.ANY)
        dma = pltpu.SemaphoreType.DMA
        return pl.pallas_call(
            moe_kernel,
            out_shape=(jax.ShapeDtypeStruct((tok_count, dim), BF16), jax.ShapeDtypeStruct((NUM_DEV, HEAD, width), BF16)),
            in_specs=[vmem, vmem, vmem, hbm, hbm, hbm],
            out_specs=(vmem, hbm),
            scratch_shapes=[
                pltpu.VMEM((NUM_DEV, HEAD, width), BF16),
                pltpu.VMEM((NUM_DEV, HEAD, width), BF16),
                pltpu.VMEM((NUM_DEV, HEAD, width), BF16),
                pltpu.VMEM((NUM_DEV, HEAD, width), BF16),
                pltpu.VMEM((dim, ff), BF16),
                pltpu.VMEM((dim, ff), BF16),
                pltpu.VMEM((ff, dim), BF16),
                pltpu.VMEM((tok_count, dim), F32),
                pltpu.VMEM((num_exp, tok_count), BF16),
                pltpu.VMEM((tok_count, num_exp), BF16),
                pltpu.VMEM((3, tok_count, num_exp), BF16),
                pltpu.VMEM((few, dim), BF16),
                pltpu.VMEM((few, ff), BF16),
                pltpu.VMEM((GROUP * HEAD, dim // PARTS), F32),
                dma((3,)),
                dma((NUM_DEV,)),
                dma((NUM_DEV,)),
                dma((NUM_DEV,)),
                dma((NUM_DEV,)),
                dma((NUM_GROUPS,)),
                dma((NUM_GROUPS,)),
                dma((NUM_GROUPS,)),
                dma((NUM_GROUPS,)),
            ],
            compiler_params=pltpu.CompilerParams(collective_id=0, has_side_effects=True, vmem_limit_bytes=63 * 2**20),
        )(tokens, w_router, routes.T, w_gate[0], w_up[0], w_down[0])[0]

    return jax.shard_map(per_device, mesh=mesh, in_specs=(row_spec, P(), row_spec, weight_spec, weight_spec, weight_spec), out_specs=row_spec, check_vma=False)
```

```python
import functools

import jax
import jax.numpy as jnp
from jax import lax
from jax.experimental import pallas as pl
from jax.experimental.pallas import tpu as pltpu
from jax.sharding import PartitionSpec as P

MESH = pl.DeviceIdType.MESH
BF16 = jnp.bfloat16
F32 = jnp.float32
NUM_DEV = 128
SHIFTS = (0, 10, 13, 7, 15, 5, 8, 2, 14, 4, 6, 12, 11, 1, 9, 3)
GROUP = 8
NUM_GROUPS = NUM_DEV // GROUP
CAPACITY = 20
HEAD = 16
TAIL = CAPACITY - HEAD
PARTS = HEAD // TAIL
FORWARD = 4
EXPERT = 6
RETURN = 8
COMBINE = 11

def iota(shape, dim):
    return lax.broadcasted_iota(jnp.int32, shape, dim)


def dot(a, b, dims=((1,), (0,))):
    return lax.dot_general(a, b, (dims, ((), ())), preferred_element_type=F32)


def moe_kernel(tokens, router, routes, gate_hbm, up_hbm, down_hbm, out, mid, send, recv, back_mid, back, w_gate, w_up, w_down, acc, place_t, place, gates, rows, hidden, tail_acc, weight_sem, send_sem, recv_sem, ret_sem, ret_mid_sem, line_sem, mid_sem, line_ret_sem, back_sem):
    tok_count, dim = tokens.shape
    num_exp = router.shape[1]
    top_k = routes.shape[0]
    part = dim // PARTS
    block = GROUP * HEAD
    outer = lax.axis_index('outer')
    line = lax.axis_index('expert')
    at_z, at_y = outer // 4, lax.rem(outer, 4)
    at_x, at_c = line // 2, lax.rem(line, 2)

    def line_shift(g):
        other = g // (2 * 4)
        n = lax.rem(g + 2 * other, 8)
        pair, last = n // 2, lax.rem(n, 2)
        odd, big = lax.rem(pair, 2), pair // 2
        return odd * (1 - big) * (1 + 2 * last) + (1 - odd) * big * (3 - 2 * last) + 2 * odd * big, other

    def line_peer(g, sign):
        shift_x, shift_c = line_shift(g)
        return {'outer': outer, 'expert': lax.rem(at_x + 4 + sign * shift_x, 4) * 2 + lax.rem(at_c + shift_c, 2)}

    def outer_at(g, i, sign, core):
        shift = SHIFTS[i] + lax.rem(g, 2) * (SHIFTS[GROUP + i] - SHIFTS[i])
        turn = sign * (1 - 2 * core)
        to_z = lax.rem(at_z + 4 + turn * (shift // 4), 4)
        to_y = lax.rem(at_y + 4 + turn * lax.rem(shift, 4), 4)
        return to_z * 4 + to_y

    def plane_peer(g, i, sign):
        return {'outer': outer_at(g, i, sign, at_c), 'expert': line}

    def experts_of(g, which):
        shift_x, shift_c = line_shift(g)
        to_c = lax.rem(at_c + shift_c, 2)
        to_line = lax.rem(at_x + shift_x, 4) * 2 + to_c
        found = jnp.zeros_like(which)
        for i in range(GROUP):
            found = jnp.where(which == i, outer_at(g, i, 1, to_c) * 8 + to_line, found)
        return found

    def copy(src, dst, sent, got, where):
        return pltpu.make_async_remote_copy(src_ref=src, dst_ref=dst, send_sem=sent, recv_sem=got, device_id=where, device_id_type=MESH)

    def span(g, first):
        return pl.ds(g * GROUP + first, GROUP - first)

    def line_out(g, first):
        return copy(send.at[span(g, first)], mid.at[span(g, first)], line_sem.at[g], mid_sem.at[g], line_peer(g, 1))

    def line_back(g, first):
        return copy(back_mid.at[span(g, first)], back.at[span(g, first)], line_ret_sem.at[g], back_sem.at[g], line_peer(g, -1))

    def final_out(k, src, where):
        return copy(src.at[k], recv.at[k], send_sem.at[k], recv_sem.at[k], where)

    def first_back(k, dst, where):
        return copy(recv.at[k], dst.at[k], ret_sem.at[k], ret_mid_sem.at[k], where)

    def by_half(g, what):
        @pl.when(lax.rem(g, 2) == 0)
        def _():
            what(1)

        @pl.when(lax.rem(g, 2) == 1)
        def _():
            what(0)

    def each(g, what):
        def step(k, carry):
            what(k)
            return carry

        lax.fori_loop(lax.max(g * GROUP, 1), g * GROUP + GROUP, step, 0)

    lines = lax.axis_size('expert')
    outers = lax.axis_size('outer')
    barrier = pltpu.get_barrier_semaphore()

    for n in range(1, lines):
        pl.semaphore_signal(barrier, inc=1, device_id={'outer': outer, 'expert': lax.rem(line + n, lines)}, device_id_type=MESH)
    for n in range(1, outers):
        pl.semaphore_signal(barrier, inc=1, device_id={'outer': lax.rem(outer + n, outers), 'expert': line}, device_id_type=MESH)
    weights = [pltpu.make_async_copy(src, dst, weight_sem.at[n]) for n, (src, dst) in enumerate(((gate_hbm, w_gate), (up_hbm, w_up), (down_hbm, w_down)))]
    for load in weights:
        load.start()

    kinds = iota((num_exp, tok_count), 0)
    chosen = routes[0:1, :] == kinds
    for j in range(1, top_k):
        chosen = chosen | (routes[j : j + 1, :] == kinds)
    square = (tok_count, tok_count)
    earlier = (iota(square, 0) < iota(square, 1)).astype(F32).astype(BF16)
    count = dot(chosen.astype(F32).astype(BF16), earlier)
    place_t[...] = jnp.where(chosen, count, -1.0).astype(BF16)

    def build(g):
        base = g * GROUP
        r = iota((block, num_exp), 0)
        pick = (experts_of(g, r >> 4) == iota((block, num_exp), 1)).astype(F32).astype(BF16)
        slots = dot(pick, place_t[...])
        r = iota((block, tok_count), 0)
        head = (slots == (r & (HEAD - 1)).astype(F32)).astype(F32).astype(BF16)
        in_tail = slots == (HEAD + (r & (TAIL - 1))).astype(F32)
        which = (r & (HEAD - 1)) >> 2
        tail_acc[...] = jnp.zeros_like(tail_acc)

        def column(q, carry):
            cols = pl.ds(pl.multiple_of(q * part, part), part)
            toks = tokens[:, cols]
            send[pl.ds(base, GROUP), :, cols] = dot(head, toks).astype(BF16).reshape(GROUP, HEAD, part)
            tail = jnp.where(in_tail & (which == q), 1.0, 0.0).astype(BF16)
            tail_acc[...] += dot(tail, toks)
            return carry

        lax.fori_loop(0, PARTS, column, 0)
        send[pl.ds(base, GROUP), :, dim:] = tail_acc[...].astype(BF16).reshape(GROUP, HEAD, part)

    def start_group(g):
        base = g * GROUP

        def direct(first):
            for i in range(first, GROUP):
                final_out(base + i, send, plane_peer(g, i, 1)).start()

        def hop(first):
            line_out(g, first).start()
            if first:
                final_out(base, send, line_peer(g, 1)).start()

        @pl.when(g < 2)
        def _():
            by_half(g, direct)

        @pl.when(g >= 2)
        def _():
            by_half(g, hop)

    def forward(g):
        def pass_on(first):
            line_out(g, first).wait_recv()
            for i in range(first, GROUP):
                final_out(g * GROUP + i, mid, plane_peer(g, i, 1)).start()

        by_half(g, pass_on)

    def find_gates():
        same = (iota(square, 0) == iota(square, 1)).astype(F32).astype(BF16)
        place[...] = dot(same, place_t[...], ((1,), (1,))).astype(BF16)
        acc[...] = jnp.zeros_like(acc)
        lanes_chosen = place[...].astype(F32) >= 0.0
        logits = dot(tokens[...], router[...])
        top = jnp.max(jnp.where(lanes_chosen, logits, -3.0e38), axis=1, keepdims=True)
        weight = jnp.where(lanes_chosen, jnp.exp(jnp.where(lanes_chosen, logits - top, 0.0)), 0.0)
        rest = weight / jnp.sum(weight, axis=1, keepdims=True)
        for n in range(3):
            term = rest.astype(BF16)
            gates[n] = term
            rest = rest - term.astype(F32)

    def run_expert(g):
        base = g * GROUP
        each(g, lambda k: final_out(k, send, line_peer(2, 1)).wait_recv())
        rows[0:block, :] = recv[pl.ds(base, GROUP), :, 0:dim].reshape(block, dim)
        tails = recv[pl.ds(base, GROUP), :, dim:].reshape(block, part)
        few = GROUP * TAIL
        i, l = iota((few, block), 0), iota((few, block), 1)
        for q in range(PARTS):
            take = (l == (i >> 2) * HEAD + q * TAIL + (i & (TAIL - 1))).astype(F32).astype(BF16)
            rows[block : block + few, q * part : (q + 1) * part] = dot(take, tails).astype(BF16)

        def up_column(n, carry):
            cols = pl.ds(pl.multiple_of(n * 256, 256), 256)
            gate = dot(rows[...], w_gate[:, cols])
            lin = dot(rows[...], w_up[:, cols])
            hidden[:, cols] = (jax.nn.silu(gate) * lin).astype(BF16)
            return carry

        lax.fori_loop(0, w_gate.shape[1] // 256, up_column, 0)
        tail_acc[...] = jnp.zeros_like(tail_acc)
        l, i = iota((block, few), 0), iota((block, few), 1)

        def down_column(q, carry):
            cols = pl.ds(pl.multiple_of(q * part, part), part)
            result = dot(hidden[...], w_down[:, cols]).astype(BF16)
            recv[pl.ds(base, GROUP), :, cols] = result[0:block].reshape(GROUP, HEAD, part)
            put = (l == (i >> 2) * HEAD + q * TAIL + (i & (TAIL - 1))).astype(F32).astype(BF16)
            tail_acc[...] += dot(put, result[block:])
            return carry

        lax.fori_loop(0, PARTS, down_column, 0)
        recv[pl.ds(base, GROUP), :, dim:] = tail_acc[...].astype(BF16).reshape(GROUP, HEAD, part)

        @pl.when(g == 0)
        def _():
            back[0] = recv[0]

        def give(first, dst):
            for i in range(first, GROUP):
                first_back(base + i, dst, plane_peer(g, i, -1)).start()

        def hop(first):
            if first:
                first_back(base, back, line_peer(g, -1)).start()
            give(first, back_mid)

        @pl.when(g < 2)
        def _():
            by_half(g, lambda first: give(first, back))

        @pl.when(g >= 2)
        def _():
            by_half(g, hop)

    def hand_on(g):
        def pass_on(first):
            for i in range(first, GROUP):
                first_back(g * GROUP + i, back_mid, line_peer(g, -1)).wait_recv()
            line_back(g, first).start()

        by_half(g, pass_on)

    def combine(g):
        base = g * GROUP
        l = iota((num_exp, block), 1)
        pick = (experts_of(g, l >> 4) == iota((num_exp, block), 0)).astype(F32).astype(BF16)
        slots = dot(place[...], pick)
        l = iota((tok_count, block), 1)
        in_head = slots == (l & (HEAD - 1)).astype(F32)
        in_tail = slots == (HEAD + (l & (TAIL - 1))).astype(F32)
        which = (l & (HEAD - 1)) >> 2
        spread = [dot(gates[n], pick) for n in range(3)]
        heads = jnp.concatenate([jnp.where(in_head, s, 0.0).astype(BF16) for s in spread], axis=0)
        tails = jnp.concatenate([jnp.where(in_tail, s, 0.0).astype(BF16) for s in spread], axis=0)
        which = jnp.concatenate([which] * 3, axis=0)

        @pl.when(g < 2)
        def _():
            each(g, lambda k: first_back(k, back, line_peer(2, -1)).wait_recv())

        def arrive(first):
            line_back(g, first).wait_recv()
            if first:
                first_back(base, back, line_peer(g, -1)).wait_recv()

        @pl.when(g >= 2)
        def _():
            by_half(g, arrive)


        def column(q, carry):
            cols = pl.ds(pl.multiple_of(q * part, part), part)
            total = dot(heads, back[pl.ds(base, GROUP), :, cols].reshape(block, part))
            mine = jnp.where(which == q, tails.astype(F32), 0.0).astype(BF16)
            total += dot(mine, back[pl.ds(base, GROUP), :, dim:].reshape(block, part))
            acc[:, cols] += total[0:tok_count] + (total[tok_count : 2 * tok_count] + total[2 * tok_count :])
            return carry

        lax.fori_loop(0, PARTS, column, 0)

    build(0)
    recv[0] = send[0]
    pl.semaphore_wait(barrier, lines + outers - 2)
    start_group(0)

    def step(i, carry):
        @pl.when((i > 0) & (i < NUM_GROUPS))
        def _():
            build(i)
            start_group(i)

        @pl.when((i >= FORWARD + 2) & (i < NUM_GROUPS + FORWARD))
        def _():
            forward(i - FORWARD)

        @pl.when(i == 2)
        def _():
            find_gates()

        @pl.when(i == EXPERT)
        def _():
            for load in weights:
                load.wait()

        @pl.when((i >= EXPERT) & (i < NUM_GROUPS + EXPERT))
        def _():
            run_expert(i - EXPERT)

        @pl.when((i >= RETURN + 2) & (i < NUM_GROUPS + RETURN))
        def _():
            hand_on(i - RETURN)

        @pl.when(i >= COMBINE)
        def _():
            combine(i - COMBINE)

        return carry

    lax.fori_loop(0, NUM_GROUPS + COMBINE, step, 0)
    out[...] = acc[...].astype(BF16)

    def drain(k, carry):
        final_out(k, send, line_peer(2, 1)).wait_send()
        first_back(k, back, line_peer(2, -1)).wait_send()
        return carry

    lax.fori_loop(1, NUM_DEV, drain, 0)

    def drain_line(g, carry):
        def drained(first):
            line_out(g, first).wait_send()
            line_back(g, first).wait_send()

        by_half(g, drained)
        return carry

    lax.fori_loop(2, NUM_GROUPS, drain_line, 0)


def solution(mesh):
    row_spec = P(('data', 'outer', 'expert'), None)
    weight_spec = P(('outer', 'expert'), None, None)

    def per_device(tokens, w_router, routes, w_gate, w_up, w_down):
        tok_count, dim = tokens.shape
        num_exp = w_router.shape[1]
        ff = w_gate.shape[2]
        width = dim + dim // PARTS
        few = GROUP * CAPACITY
        vmem = pl.BlockSpec(memory_space=pltpu.VMEM)
        hbm = pl.BlockSpec(memory_space=pl.ANY)
        dma = pltpu.SemaphoreType.DMA
        return pl.pallas_call(
            moe_kernel,
            out_shape=(jax.ShapeDtypeStruct((tok_count, dim), BF16), jax.ShapeDtypeStruct((NUM_DEV, HEAD, width), BF16)),
            in_specs=[vmem, vmem, vmem, hbm, hbm, hbm],
            out_specs=(vmem, hbm),
            scratch_shapes=[
                pltpu.VMEM((NUM_DEV, HEAD, width), BF16),
                pltpu.VMEM((NUM_DEV, HEAD, width), BF16),
                pltpu.VMEM((NUM_DEV, HEAD, width), BF16),
                pltpu.VMEM((NUM_DEV, HEAD, width), BF16),
                pltpu.VMEM((dim, ff), BF16),
                pltpu.VMEM((dim, ff), BF16),
                pltpu.VMEM((ff, dim), BF16),
                pltpu.VMEM((tok_count, dim), F32),
                pltpu.VMEM((num_exp, tok_count), BF16),
                pltpu.VMEM((tok_count, num_exp), BF16),
                pltpu.VMEM((3, tok_count, num_exp), BF16),
                pltpu.VMEM((few, dim), BF16),
                pltpu.VMEM((few, ff), BF16),
                pltpu.VMEM((GROUP * HEAD, dim // PARTS), F32),
                dma((3,)),
                dma((NUM_DEV,)),
                dma((NUM_DEV,)),
                dma((NUM_DEV,)),
                dma((NUM_DEV,)),
                dma((NUM_GROUPS,)),
                dma((NUM_GROUPS,)),
                dma((NUM_GROUPS,)),
                dma((NUM_GROUPS,)),
            ],
            compiler_params=pltpu.CompilerParams(collective_id=0, has_side_effects=True, vmem_limit_bytes=63 * 2**20),
        )(tokens, w_router, routes.T, w_gate[0], w_up[0], w_down[0])[0]

    return jax.shard_map(per_device, mesh=mesh, in_specs=(row_spec, P(), row_spec, weight_spec, weight_spec, weight_spec), out_specs=row_spec, check_vma=False)
```

```python
import functools

import jax
import jax.numpy as jnp
from jax import lax
from jax.experimental import pallas as pl
from jax.experimental.pallas import tpu as pltpu
from jax.sharding import PartitionSpec as P

MESH = pl.DeviceIdType.MESH
BF16 = jnp.bfloat16
F32 = jnp.float32
NUM_DEV = 128
SHIFTS = (0, 10, 13, 7, 15, 5, 8, 2, 14, 4, 6, 12, 11, 1, 9, 3)
GROUP = 8
NUM_GROUPS = NUM_DEV // GROUP
CAPACITY = 20
HEAD = 16
TAIL = CAPACITY - HEAD
PARTS = HEAD // TAIL
FORWARD = 4
EXPERT = 6
RETURN = 8
COMBINE = 11

def iota(shape, dim):
    return lax.broadcasted_iota(jnp.int32, shape, dim)


def dot(a, b, dims=((1,), (0,))):
    return lax.dot_general(a, b, (dims, ((), ())), preferred_element_type=F32)


def moe_kernel(tokens, router, routes, gate_hbm, up_hbm, down_hbm, out, mid, send, recv, back_mid, back, w_gate, w_up, w_down, acc, place_t, place, gates, rows, hidden, tail_acc, weight_sem, send_sem, recv_sem, ret_sem, ret_mid_sem, line_sem, mid_sem, line_ret_sem, back_sem):
    tok_count, dim = tokens.shape
    num_exp = router.shape[1]
    top_k = routes.shape[0]
    part = dim // PARTS
    block = GROUP * HEAD
    outer = lax.axis_index('outer')
    line = lax.axis_index('expert')
    at_z, at_y = outer // 4, lax.rem(outer, 4)
    at_x, at_c = line // 2, lax.rem(line, 2)

    def line_shift(g):
        other = g // (2 * 4)
        n = lax.rem(g + 2 * other, 8)
        pair, last = n // 2, lax.rem(n, 2)
        odd, big = lax.rem(pair, 2), pair // 2
        return odd * (1 - big) * (1 + 2 * last) + (1 - odd) * big * (3 - 2 * last) + 2 * odd * big, other

    def line_peer(g, sign):
        shift_x, shift_c = line_shift(g)
        return {'outer': outer, 'expert': lax.rem(at_x + 4 + sign * shift_x, 4) * 2 + lax.rem(at_c + shift_c, 2)}

    def outer_at(g, i, sign, core):
        shift = SHIFTS[i] + lax.rem(g, 2) * (SHIFTS[GROUP + i] - SHIFTS[i])
        turn = sign * (1 - 2 * core)
        to_z = lax.rem(at_z + 4 + turn * (shift // 4), 4)
        to_y = lax.rem(at_y + 4 + turn * lax.rem(shift, 4), 4)
        return to_z * 4 + to_y

    def plane_peer(g, i, sign):
        return {'outer': outer_at(g, i, sign, at_c), 'expert': line}

    def experts_of(g, which):
        shift_x, shift_c = line_shift(g)
        to_c = lax.rem(at_c + shift_c, 2)
        to_line = lax.rem(at_x + shift_x, 4) * 2 + to_c
        found = jnp.zeros_like(which)
        for i in range(GROUP):
            found = jnp.where(which == i, outer_at(g, i, 1, to_c) * 8 + to_line, found)
        return found

    def copy(src, dst, sent, got, where):
        return pltpu.make_async_remote_copy(src_ref=src, dst_ref=dst, send_sem=sent, recv_sem=got, device_id=where, device_id_type=MESH)

    def span(g, first):
        return pl.ds(g * GROUP + first, GROUP - first)

    def line_out(g, first):
        return copy(send.at[span(g, first)], mid.at[span(g, first)], line_sem.at[g], mid_sem.at[g], line_peer(g, 1))

    def line_back(g, first):
        return copy(back_mid.at[span(g, first)], back.at[span(g, first)], line_ret_sem.at[g], back_sem.at[g], line_peer(g, -1))

    def final_out(k, src, where):
        return copy(src.at[k], recv.at[k], send_sem.at[k], recv_sem.at[k], where)

    def first_back(k, dst, where):
        return copy(recv.at[k], dst.at[k], ret_sem.at[k], ret_mid_sem.at[k], where)

    def by_half(g, what):
        @pl.when(lax.rem(g, 2) == 0)
        def _():
            what(1)

        @pl.when(lax.rem(g, 2) == 1)
        def _():
            what(0)

    def each(g, what):
        def step(k, carry):
            what(k)
            return carry

        lax.fori_loop(lax.max(g * GROUP, 1), g * GROUP + GROUP, step, 0)

    lines = lax.axis_size('expert')
    outers = lax.axis_size('outer')
    barrier = pltpu.get_barrier_semaphore()

    for n in range(1, lines):
        pl.semaphore_signal(barrier, inc=1, device_id={'outer': outer, 'expert': lax.rem(line + n, lines)}, device_id_type=MESH)
    for n in range(1, outers):
        pl.semaphore_signal(barrier, inc=1, device_id={'outer': lax.rem(outer + n, outers), 'expert': line}, device_id_type=MESH)
    weights = [pltpu.make_async_copy(src, dst, weight_sem.at[n]) for n, (src, dst) in enumerate(((gate_hbm, w_gate), (up_hbm, w_up), (down_hbm, w_down)))]
    for load in weights:
        load.start()

    kinds = iota((num_exp, tok_count), 0)
    chosen = routes[0:1, :] == kinds
    for j in range(1, top_k):
        chosen = chosen | (routes[j : j + 1, :] == kinds)
    square = (tok_count, tok_count)
    earlier = (iota(square, 0) < iota(square, 1)).astype(F32).astype(BF16)
    count = dot(chosen.astype(F32).astype(BF16), earlier)
    place_t[...] = jnp.where(chosen, count, -1.0).astype(BF16)

    def build(g):
        base = g * GROUP
        r = iota((block, num_exp), 0)
        pick = (experts_of(g, r >> 4) == iota((block, num_exp), 1)).astype(F32).astype(BF16)
        slots = dot(pick, place_t[...])
        r = iota((block, tok_count), 0)
        head = (slots == (r & (HEAD - 1)).astype(F32)).astype(F32).astype(BF16)
        in_tail = slots == (HEAD + (r & (TAIL - 1))).astype(F32)
        which = (r & (HEAD - 1)) >> 2
        tail_acc[...] = jnp.zeros_like(tail_acc)

        def column(q, carry):
            cols = pl.ds(pl.multiple_of(q * part, part), part)
            toks = tokens[:, cols]
            send[pl.ds(base, GROUP), :, cols] = dot(head, toks).astype(BF16).reshape(GROUP, HEAD, part)
            tail = jnp.where(in_tail & (which == q), 1.0, 0.0).astype(BF16)
            tail_acc[...] += dot(tail, toks)
            return carry

        lax.fori_loop(0, PARTS, column, 0)
        send[pl.ds(base, GROUP), :, dim:] = tail_acc[...].astype(BF16).reshape(GROUP, HEAD, part)

    def start_group(g):
        base = g * GROUP

        def direct(first):
            for i in range(first, GROUP):
                final_out(base + i, send, plane_peer(g, i, 1)).start()

        def hop(first):
            line_out(g, first).start()
            if first:
                final_out(base, send, line_peer(g, 1)).start()

        @pl.when(g < 2)
        def _():
            by_half(g, direct)

        @pl.when(g >= 2)
        def _():
            by_half(g, hop)

    def forward(g):
        def pass_on(first):
            line_out(g, first).wait_recv()
            for i in range(first, GROUP):
                final_out(g * GROUP + i, mid, plane_peer(g, i, 1)).start()

        by_half(g, pass_on)

    def find_gates():
        same = (iota(square, 0) == iota(square, 1)).astype(F32).astype(BF16)
        place[...] = dot(same, place_t[...], ((1,), (1,))).astype(BF16)
        acc[...] = jnp.zeros_like(acc)
        lanes_chosen = place[...].astype(F32) >= 0.0
        logits = dot(tokens[...], router[...])
        top = jnp.max(jnp.where(lanes_chosen, logits, -3.0e38), axis=1, keepdims=True)
        weight = jnp.where(lanes_chosen, jnp.exp(jnp.where(lanes_chosen, logits - top, 0.0)), 0.0)
        rest = weight / jnp.sum(weight, axis=1, keepdims=True)
        for n in range(3):
            term = rest.astype(BF16)
            gates[n] = term
            rest = rest - term.astype(F32)

    def run_expert(g):
        base = g * GROUP
        each(g, lambda k: final_out(k, send, line_peer(2, 1)).wait_recv())
        rows[0:block, :] = recv[pl.ds(base, GROUP), :, 0:dim].reshape(block, dim)
        tails = recv[pl.ds(base, GROUP), :, dim:].reshape(block, part)
        few = GROUP * TAIL
        i, l = iota((few, block), 0), iota((few, block), 1)
        for q in range(PARTS):
            take = (l == (i >> 2) * HEAD + q * TAIL + (i & (TAIL - 1))).astype(F32).astype(BF16)
            rows[block : block + few, q * part : (q + 1) * part] = dot(take, tails).astype(BF16)

        def up_column(n, carry):
            cols = pl.ds(pl.multiple_of(n * 256, 256), 256)
            gate = dot(rows[...], w_gate[:, cols])
            lin = dot(rows[...], w_up[:, cols])
            hidden[:, cols] = (jax.nn.silu(gate) * lin).astype(BF16)
            return carry

        lax.fori_loop(0, w_gate.shape[1] // 256, up_column, 0)
        tail_acc[...] = jnp.zeros_like(tail_acc)
        l, i = iota((block, few), 0), iota((block, few), 1)

        def down_column(q, carry):
            cols = pl.ds(pl.multiple_of(q * part, part), part)
            result = dot(hidden[...], w_down[:, cols]).astype(BF16)
            recv[pl.ds(base, GROUP), :, cols] = result[0:block].reshape(GROUP, HEAD, part)
            put = (l == (i >> 2) * HEAD + q * TAIL + (i & (TAIL - 1))).astype(F32).astype(BF16)
            tail_acc[...] += dot(put, result[block:])
            return carry

        lax.fori_loop(0, PARTS, down_column, 0)
        recv[pl.ds(base, GROUP), :, dim:] = tail_acc[...].astype(BF16).reshape(GROUP, HEAD, part)

        @pl.when(g == 0)
        def _():
            back[0] = recv[0]

        def give(first, dst):
            for i in range(first, GROUP):
                first_back(base + i, dst, plane_peer(g, i, -1)).start()

        def hop(first):
            if first:
                first_back(base, back, line_peer(g, -1)).start()
            give(first, back_mid)

        @pl.when(g < 2)
        def _():
            by_half(g, lambda first: give(first, back))

        @pl.when(g >= 2)
        def _():
            by_half(g, hop)

    def hand_on(g):
        def pass_on(first):
            for i in range(first, GROUP):
                first_back(g * GROUP + i, back_mid, line_peer(g, -1)).wait_recv()
            line_back(g, first).start()

        by_half(g, pass_on)

    def combine(g):
        base = g * GROUP
        l = iota((num_exp, block), 1)
        pick = (experts_of(g, l >> 4) == iota((num_exp, block), 0)).astype(F32).astype(BF16)
        slots = dot(place[...], pick)
        l = iota((tok_count, block), 1)
        in_head = slots == (l & (HEAD - 1)).astype(F32)
        in_tail = slots == (HEAD + (l & (TAIL - 1))).astype(F32)
        which = (l & (HEAD - 1)) >> 2
        spread = [dot(gates[n], pick) for n in range(3)]
        heads = jnp.concatenate([jnp.where(in_head, s, 0.0).astype(BF16) for s in spread], axis=0)
        tails = jnp.concatenate([jnp.where(in_tail, s, 0.0).astype(BF16) for s in spread], axis=0)
        which = jnp.concatenate([which] * 3, axis=0)

        def drain(k):
            final_out(k, send, line_peer(2, 1)).wait_send()
            first_back(k, back, line_peer(2, -1)).wait_send()

        def drain_line(first):
            line_out(g, first).wait_send()
            line_back(g, first).wait_send()

        each(g, drain)

        @pl.when(g >= 2)
        def _():
            by_half(g, drain_line)

        @pl.when(g < 2)
        def _():
            each(g, lambda k: first_back(k, back, line_peer(2, -1)).wait_recv())

        def arrive(first):
            line_back(g, first).wait_recv()
            if first:
                first_back(base, back, line_peer(g, -1)).wait_recv()

        @pl.when(g >= 2)
        def _():
            by_half(g, arrive)


        def column(q, carry):
            cols = pl.ds(pl.multiple_of(q * part, part), part)
            total = dot(heads, back[pl.ds(base, GROUP), :, cols].reshape(block, part))
            mine = jnp.where(which == q, tails.astype(F32), 0.0).astype(BF16)
            total += dot(mine, back[pl.ds(base, GROUP), :, dim:].reshape(block, part))
            acc[:, cols] += total[0:tok_count] + (total[tok_count : 2 * tok_count] + total[2 * tok_count :])
            return carry

        lax.fori_loop(0, PARTS, column, 0)

    build(0)
    recv[0] = send[0]
    pl.semaphore_wait(barrier, lines + outers - 2)
    start_group(0)

    def step(i, carry):
        @pl.when((i > 0) & (i < NUM_GROUPS))
        def _():
            build(i)
            start_group(i)

        @pl.when((i >= FORWARD + 2) & (i < NUM_GROUPS + FORWARD))
        def _():
            forward(i - FORWARD)

        @pl.when(i == 2)
        def _():
            find_gates()

        @pl.when(i == EXPERT)
        def _():
            for load in weights:
                load.wait()

        @pl.when((i >= EXPERT) & (i < NUM_GROUPS + EXPERT))
        def _():
            run_expert(i - EXPERT)

        @pl.when((i >= RETURN + 2) & (i < NUM_GROUPS + RETURN))
        def _():
            hand_on(i - RETURN)

        @pl.when(i >= COMBINE)
        def _():
            combine(i - COMBINE)

        return carry

    lax.fori_loop(0, NUM_GROUPS + COMBINE, step, 0)
    out[...] = acc[...].astype(BF16)


def solution(mesh):
    row_spec = P(('data', 'outer', 'expert'), None)
    weight_spec = P(('outer', 'expert'), None, None)

    def per_device(tokens, w_router, routes, w_gate, w_up, w_down):
        tok_count, dim = tokens.shape
        num_exp = w_router.shape[1]
        ff = w_gate.shape[2]
        width = dim + dim // PARTS
        few = GROUP * CAPACITY
        vmem = pl.BlockSpec(memory_space=pltpu.VMEM)
        hbm = pl.BlockSpec(memory_space=pl.ANY)
        dma = pltpu.SemaphoreType.DMA
        return pl.pallas_call(
            moe_kernel,
            out_shape=(jax.ShapeDtypeStruct((tok_count, dim), BF16), jax.ShapeDtypeStruct((NUM_DEV, HEAD, width), BF16)),
            in_specs=[vmem, vmem, vmem, hbm, hbm, hbm],
            out_specs=(vmem, hbm),
            scratch_shapes=[
                pltpu.VMEM((NUM_DEV, HEAD, width), BF16),
                pltpu.VMEM((NUM_DEV, HEAD, width), BF16),
                pltpu.VMEM((NUM_DEV, HEAD, width), BF16),
                pltpu.VMEM((NUM_DEV, HEAD, width), BF16),
                pltpu.VMEM((dim, ff), BF16),
                pltpu.VMEM((dim, ff), BF16),
                pltpu.VMEM((ff, dim), BF16),
                pltpu.VMEM((tok_count, dim), F32),
                pltpu.VMEM((num_exp, tok_count), BF16),
                pltpu.VMEM((tok_count, num_exp), BF16),
                pltpu.VMEM((3, tok_count, num_exp), BF16),
                pltpu.VMEM((few, dim), BF16),
                pltpu.VMEM((few, ff), BF16),
                pltpu.VMEM((GROUP * HEAD, dim // PARTS), F32),
                dma((3,)),
                dma((NUM_DEV,)),
                dma((NUM_DEV,)),
                dma((NUM_DEV,)),
                dma((NUM_DEV,)),
                dma((NUM_GROUPS,)),
                dma((NUM_GROUPS,)),
                dma((NUM_GROUPS,)),
                dma((NUM_GROUPS,)),
            ],
            compiler_params=pltpu.CompilerParams(collective_id=0, has_side_effects=True, vmem_limit_bytes=63 * 2**20),
        )(tokens, w_router, routes.T, w_gate[0], w_up[0], w_down[0])[0]

    return jax.shard_map(per_device, mesh=mesh, in_specs=(row_spec, P(), row_spec, weight_spec, weight_spec, weight_spec), out_specs=row_spec, check_vma=False)
```
